16 devices in a mesh: dp: 2 (over y, z), cp: 8 (over x, core).
Axes of the slice: x: 4, y: 2, z: 1, core: 2. Of those that a mesh axis runs over, the one named last changes fastest.
The devices are a block of a 4x4x8 slice.
Arguments:
- x_in: bfloat16 [24, 3072, 1536], P('dp', 'cp'), parts along dimension 0
- grad_y: bfloat16 [24, 3072, 1536], P('dp', 'cp'), parts along dimension 0
- positions: int32 [24, 3072], P('dp', 'cp'), parts along dimension 0
- seg_ids: int32 [24, 3072], P('dp', 'cp'), parts along dimension 0
- norm_gain: bfloat16 [1536], replicated
- w_q: bfloat16 [1536, 1536], replicated
- b_q: bfloat16 [1536], replicated
- w_k: bfloat16 [1536, 256], replicated
- b_k: bfloat16 [256], replicated
- w_v: bfloat16 [1536, 256], replicated
- b_v: bfloat16 [256], replicated
- w_o: bfloat16 [1536, 1536], replicated
Outputs:
- output 1: bfloat16 [24, 3072, 1536], P('dp', 'cp'), parts along dimension 0
- output 2: bfloat16 [24, 3072, 1536], P('dp', 'cp'), parts along dimension 0
- output 3: float32 [3072], P('dp'), parts along dimension 0
- output 4: float32 [3072, 1536], P('dp'), parts along dimension 0
- output 5: float32 [3072], P('dp'), parts along dimension 0
- output 6: float32 [3072, 256], P('dp'), parts along dimension 0
- output 7: float32 [512], P('dp'), parts along dimension 0
- output 8: float32 [3072, 256], P('dp'), parts along dimension 0
- output 9: float32 [512], P('dp'), parts along dimension 0
- output 10: float32 [3072, 1536], P('dp'), parts along dimension 0
There are 2 independent parts. The reference program is written for one: setup_inputs(seed, part) draws one part's arguments, and reference() takes and returns one part's arrays. A program takes and returns all parts, laid end to end along the dimension named above; an argument that names none is the same for every part.
All inputs are finite; a program needn't handle non-finite values.
Results may differ from the reference program's by a relative error of at most 0.0193444.
Values are sent between devices in bfloat16 or wider.
A program may use at most 768 MiB of HBM per device.

```python
import jax
import jax.numpy as jnp
from jax import lax

D = 1536
HEADS = 12
KV_HEADS = 2
HEAD = 128
BATCH = 12
SEQ = 3072
QUERY_BLOCK = 64
DOC_CUTS = 3

THETA = 1000000.0
EPS = 1e-6
KV_WIDTH = KV_HEADS * HEAD
GROUP = HEADS // KV_HEADS


def draw_documents(doc_key):
    cuts = jax.random.randint(doc_key, (BATCH, DOC_CUTS), 1, SEQ)
    token_index = jnp.arange(SEQ, dtype=jnp.int32)
    passed = token_index[None, :, None] >= cuts[:, None, :]
    seg_ids = jnp.sum(passed.astype(jnp.int32), axis=-1)
    doc_start = jnp.max(jnp.where(passed, cuts[:, None, :], 0), axis=-1)
    positions = token_index[None, :] - doc_start
    return positions.astype(jnp.int32), seg_ids.astype(jnp.int32)


def setup_inputs(seed: int = 0, part: int = 0) -> dict:
    part_keys = jax.random.split(jax.random.fold_in(jax.random.key(seed), part), 3)
    shared_keys = jax.random.split(jax.random.key(seed + 1), 8)
    positions, seg_ids = draw_documents(part_keys[2])
    fan_scale = D ** -0.5
    x_in = jax.random.normal(part_keys[0], (BATCH, SEQ, D), jnp.float32)
    grad_y = jax.random.normal(part_keys[1], (BATCH, SEQ, D), jnp.float32)
    norm_gain = 1.0 + 0.3 * jax.random.normal(shared_keys[0], (D,), jnp.float32)
    w_q = fan_scale * jax.random.normal(shared_keys[1], (D, D), jnp.float32)
    b_q = 0.5 * jax.random.normal(shared_keys[2], (D,), jnp.float32)
    w_k = fan_scale * jax.random.normal(shared_keys[3], (D, KV_WIDTH), jnp.float32)
    b_k = 1.5 * jax.random.normal(shared_keys[4], (KV_WIDTH,), jnp.float32)
    w_v = fan_scale * jax.random.normal(shared_keys[5], (D, KV_WIDTH), jnp.float32)
    b_v = 0.3 * jax.random.normal(shared_keys[6], (KV_WIDTH,), jnp.float32)
    w_o = fan_scale * jax.random.normal(shared_keys[7], (D, D), jnp.float32)
    return {
        'x_in': x_in.astype(jnp.bfloat16),
        'grad_y': grad_y.astype(jnp.bfloat16),
        'positions': positions,
        'seg_ids': seg_ids,
        'norm_gain': norm_gain.astype(jnp.bfloat16),
        'w_q': w_q.astype(jnp.bfloat16),
        'b_q': b_q.astype(jnp.bfloat16),
        'w_k': w_k.astype(jnp.bfloat16),
        'b_k': b_k.astype(jnp.bfloat16),
        'w_v': w_v.astype(jnp.bfloat16),
        'b_v': b_v.astype(jnp.bfloat16),
        'w_o': w_o.astype(jnp.bfloat16),
    }


def rope_tables(positions):
    inv_freq = THETA ** (-jnp.arange(0, HEAD, 2).astype(jnp.float32) / HEAD)
    angles = positions.astype(jnp.float32)[..., None] * inv_freq
    angles = jnp.concatenate([angles, angles], axis=-1)
    return jnp.cos(angles), jnp.sin(angles)


def rotate(values, cos_t, sin_t):
    half_head = HEAD // 2
    turned = jnp.concatenate([-values[..., half_head:], values[..., :half_head]], axis=-1)
    return values * cos_t + turned * sin_t


def unrotate(grad_in, cos_t, sin_t):
    half_head = HEAD // 2
    scaled = grad_in * sin_t
    return grad_in * cos_t + jnp.concatenate([scaled[..., half_head:], -scaled[..., :half_head]], axis=-1)


def reference(x_in, grad_y, positions, seg_ids, norm_gain, w_q, b_q, w_k, b_k, w_v, b_v, w_o):
    tokens = BATCH * SEQ
    scale = HEAD ** -0.5
    x_wide = x_in.astype(jnp.float32).reshape(tokens, D)
    dy_flat = grad_y.reshape(tokens, D)
    inv_rms = lax.rsqrt(jnp.mean(x_wide * x_wide, axis=-1, keepdims=True) + EPS)
    gain = norm_gain.astype(jnp.float32)
    normed = (x_wide * inv_rms * gain).astype(jnp.bfloat16)
    cos_t, sin_t = rope_tables(positions)
    cos_h = cos_t[:, :, None, :]
    sin_h = sin_t[:, :, None, :]
    q_lin = (jnp.dot(normed, w_q, preferred_element_type=jnp.float32) + b_q.astype(jnp.float32)).reshape(BATCH, SEQ, HEADS, HEAD)
    k_lin = (jnp.dot(normed, w_k, preferred_element_type=jnp.float32) + b_k.astype(jnp.float32)).reshape(BATCH, SEQ, KV_HEADS, HEAD)
    v_lin = jnp.dot(normed, w_v, preferred_element_type=jnp.float32) + b_v.astype(jnp.float32)
    queries = rotate(q_lin, cos_h, sin_h).astype(jnp.bfloat16).reshape(BATCH, SEQ, KV_HEADS, GROUP, HEAD)
    queries = jnp.transpose(queries, (0, 2, 3, 1, 4)).astype(jnp.float32)
    keys_wide = rotate(k_lin, cos_h, sin_h).astype(jnp.bfloat16).astype(jnp.float32)
    values_wide = v_lin.astype(jnp.bfloat16).astype(jnp.float32).reshape(BATCH, SEQ, KV_HEADS, HEAD)
    d_attn = jnp.dot(dy_flat, w_o.T, preferred_element_type=jnp.float32).astype(jnp.bfloat16)
    d_attn = jnp.transpose(d_attn.reshape(BATCH, SEQ, KV_HEADS, GROUP, HEAD), (0, 2, 3, 1, 4)).astype(jnp.float32)
    key_index = jnp.arange(SEQ)
    num_blocks = SEQ // QUERY_BLOCK

    def block_step(carry, block):
        dk_acc, dv_acc = carry
        start = block * QUERY_BLOCK
        q_blk = lax.dynamic_slice_in_dim(queries, start, QUERY_BLOCK, 3)
        da_blk = lax.dynamic_slice_in_dim(d_attn, start, QUERY_BLOCK, 3)
        seg_blk = lax.dynamic_slice_in_dim(seg_ids, start, QUERY_BLOCK, 1)
        query_index = start + jnp.arange(QUERY_BLOCK)
        allowed = (key_index[None, None, :] <= query_index[None, :, None]) & (seg_blk[:, :, None] == seg_ids[:, None, :])
        scores = jnp.einsum('bkgqd,bskd->bkgqs', q_blk, keys_wide) * scale
        scores = jnp.where(allowed[:, None, None], scores, -jnp.inf)
        row_max = jnp.max(scores, axis=-1, keepdims=True)
        weights = jnp.exp(scores - row_max)
        row_sum = jnp.sum(weights, axis=-1, keepdims=True)
        attn_out = jnp.einsum('bkgqs,bskd->bkgqd', weights.astype(jnp.bfloat16).astype(jnp.float32), values_wide) / row_sum
        attn_out = attn_out.astype(jnp.bfloat16).astype(jnp.float32)
        attn_prob = weights / row_sum
        d_probs = jnp.einsum('bkgqd,bskd->bkgqs', da_blk, values_wide)
        delta = jnp.sum(da_blk * attn_out, axis=-1, keepdims=True)
        d_scores = (attn_prob * (d_probs - delta)).astype(jnp.bfloat16).astype(jnp.float32)
        dq_blk = jnp.einsum('bkgqs,bskd->bkgqd', d_scores, keys_wide) * scale
        dk_acc = dk_acc + jnp.einsum('bkgqs,bkgqd->bskd', d_scores, q_blk) * scale
        dv_acc = dv_acc + jnp.einsum('bkgqs,bkgqd->bskd', attn_prob.astype(jnp.bfloat16).astype(jnp.float32), da_blk)
        return (dk_acc, dv_acc), (attn_out, dq_blk)

    kv_zero = jnp.zeros((BATCH, SEQ, KV_HEADS, HEAD), jnp.float32)
    (dk_acc, dv_acc), (attn_stack, dq_stack) = lax.scan(block_step, (kv_zero, kv_zero), jnp.arange(num_blocks))
    attn_flat = jnp.transpose(attn_stack, (1, 0, 4, 2, 3, 5)).reshape(tokens, D).astype(jnp.bfloat16)
    dq_heads = jnp.transpose(dq_stack, (1, 0, 4, 2, 3, 5)).reshape(BATCH, SEQ, HEADS, HEAD)
    dq_pre = unrotate(dq_heads, cos_h, sin_h).reshape(tokens, D)
    dk_pre = unrotate(dk_acc, cos_h, sin_h).reshape(tokens, KV_WIDTH)
    dv_pre = dv_acc.reshape(tokens, KV_WIDTH)
    y_out = (x_wide + jnp.dot(attn_flat, w_o, preferred_element_type=jnp.float32)).astype(jnp.bfloat16).reshape(BATCH, SEQ, D)
    dq_low = dq_pre.astype(jnp.bfloat16)
    dk_low = dk_pre.astype(jnp.bfloat16)
    dv_low = dv_pre.astype(jnp.bfloat16)
    grad_w_q = jnp.dot(normed.T, dq_low, preferred_element_type=jnp.float32)
    grad_w_k = jnp.dot(normed.T, dk_low, preferred_element_type=jnp.float32)
    grad_w_v = jnp.dot(normed.T, dv_low, preferred_element_type=jnp.float32)
    grad_w_o = jnp.dot(attn_flat.T, dy_flat, preferred_element_type=jnp.float32)
    d_normed = (jnp.dot(dq_low, w_q.T, preferred_element_type=jnp.float32)
                + jnp.dot(dk_low, w_k.T, preferred_element_type=jnp.float32)
                + jnp.dot(dv_low, w_v.T, preferred_element_type=jnp.float32))
    grad_gain = jnp.sum(d_normed * x_wide * inv_rms, axis=0)
    d_scaled = d_normed * gain
    d_x = inv_rms * (d_scaled - x_wide * inv_rms * inv_rms * jnp.mean(d_scaled * x_wide, axis=-1, keepdims=True))
    grad_x = (dy_flat.astype(jnp.float32) + d_x).astype(jnp.bfloat16).reshape(BATCH, SEQ, D)
    return (y_out, grad_x, grad_gain, grad_w_q, jnp.sum(dq_pre, axis=0), grad_w_k, jnp.sum(dk_pre, axis=0), grad_w_v, jnp.sum(dv_pre, axis=0), grad_w_o)
```

```python
import functools

import jax
import jax.numpy as jnp
from jax import lax
from jax.experimental import pallas as pl
from jax.experimental.pallas import tpu as pltpu
from jax.sharding import PartitionSpec as P

HEAD = 128
THETA = 1000000.0
EPS = 1e-6
LOG2E = 1.4426950408889634
CHUNK = 3
TILE = 128
KBLK = 256


NT = (((1,), (1,)), ((), ()))
TN = (((0,), (0,)), ((), ()))


def dot(a, b, dims=None):
    if dims is None:
        return jnp.dot(a, b, preferred_element_type=jnp.float32)
    return lax.dot_general(a, b, dims, preferred_element_type=jnp.float32)


def params(vmem_mib, dims):
    return pltpu.CompilerParams(vmem_limit_bytes=vmem_mib * 1024 * 1024, dimension_semantics=("arbitrary",) * dims)


def rotate(block, cs):
    return block * cs[:, :HEAD] + pltpu.roll(block, HEAD // 2, 1) * cs[:, HEAD:]


def unrotate(block, cs):
    return block * cs[:, :HEAD] + pltpu.roll(block * cs[:, HEAD:], HEAD // 2, 1)


def fold_rows(block):
    rows, cols = block.shape
    return jnp.sum(block.reshape(rows // 8, 8, cols), axis=0)


def projection_kernel(core_ref, xo_ref, xp_ref, go_ref, gp_ref, cs_ref, gain_ref, wq_ref, wkv_ref, wo_ref, bq_ref, bkv_ref,
                      h_ref, q_ref, da_ref, kv_ref):
    role = pl.program_id(0)

    def work(x_ref, g_ref):
        x = x_ref[0].astype(jnp.float32)
        inv = lax.rsqrt(jnp.mean(x * x, axis=-1, keepdims=True) + EPS)
        h = (x * inv * gain_ref[...]).astype(jnp.bfloat16)
        h_ref[0, 0] = h
        cs = cs_ref[0, 0]
        kv = dot(h, wkv_ref[...]) + bkv_ref[...]
        kv_ref[0, :, :HEAD] = rotate(kv[:, :HEAD], cs).astype(jnp.bfloat16)
        kv_ref[0, :, HEAD:] = kv[:, HEAD:].astype(jnp.bfloat16)
        q = dot(h, wq_ref[...]) + bq_ref[...]
        for j in range(q.shape[1] // HEAD):
            cols = slice(j * HEAD, (j + 1) * HEAD)
            q_ref[0, 0, j] = rotate(q[:, cols], cs).astype(jnp.bfloat16)
        da = dot(g_ref[0], wo_ref[...], NT).astype(jnp.bfloat16)
        for j in range(q.shape[1] // HEAD):
            da_ref[0, 0, j] = da[:, j * HEAD:(j + 1) * HEAD]

    @pl.when(role == 0)
    def _():
        work(xo_ref, go_ref)

    @pl.when(role == 1)
    def _():
        work(xp_ref, gp_ref)


def projection(core, x_own, x_oth, g_own, g_oth, cs, gain, wq, wkv, wo, bq, bkv):
    n, rows, width = x_own.shape
    qw = wq.shape[1]
    own = lambda r, b, c: (jnp.where(r == 0, b, n - 1), 0, 0)
    oth = lambda r, b, c: (jnp.where(r == 0, 0, b), 0, 0)
    role = lambda r, b, c: (r, b, 0, 0)
    half = lambda r, b, c: (b, jnp.where(r == 0, c[0], 1 - c[0]), 0)
    full = lambda r, b, c: (0, 0)
    x_spec = lambda f: pl.BlockSpec((1, rows, width), f)
    const = lambda a: pl.BlockSpec(a.shape, full, pipeline_mode=pl.Buffered(1))
    bf = jnp.bfloat16
    heads = qw // HEAD
    head_spec = pl.BlockSpec((1, 1, heads, rows, HEAD), lambda r, b, c: (r, b, 0, 0, 0))
    flops = 2 * 2 * n * rows * width * (2 * qw + 256)
    return pl.pallas_call(
        projection_kernel,
        grid_spec=pltpu.PrefetchScalarGridSpec(
            num_scalar_prefetch=1,
            grid=(2, n),
            in_specs=[x_spec(own), x_spec(oth), x_spec(own), x_spec(oth), pl.BlockSpec((1, 1, rows, 2 * HEAD), role),
                      const(gain), const(wq), const(wkv), const(wo), const(bq), const(bkv)],
            out_specs=[pl.BlockSpec((1, 1, rows, width), role), head_spec, head_spec, pl.BlockSpec((1, rows, 2 * HEAD), half)],
        ),
        out_shape=[jax.ShapeDtypeStruct((2, n, rows, width), bf), jax.ShapeDtypeStruct((2, n, heads, rows, HEAD), bf),
                   jax.ShapeDtypeStruct((2, n, heads, rows, HEAD), bf), jax.ShapeDtypeStruct((n, 2 * rows, 2 * HEAD), bf)],
        compiler_params=params(56, 2),
        cost_estimate=pl.CostEstimate(flops=flops, bytes_accessed=2 * n * rows * (3 * width + 2 * qw) * 2, transcendentals=0),
        name="projection",
    )(core, x_own, x_oth, g_own, g_oth, cs, gain, wq, wkv, wo, bq, bkv)


def attention_kernel(heads, window, core_ref, lo_ref, q_ref, da_ref, cs_ref, lov_ref, kv0_ref, kv1_ref, kv2_ref, kv3_ref,
                     ao_ref, ap_ref, dqo_ref, dqp_ref, db_ref, g0_ref, g1_ref, g2_ref, g3_ref,
                     kv_s, kvt_s, acc_s, qt_s, dat_s, p_s, sh_s, l_s, o_s, dl_s, dq_s, kn_s):
    b, role, i = pl.program_id(0), pl.program_id(1), pl.program_id(2)
    n_tiles = pl.num_programs(2)
    chip_rows = kv0_ref.shape[1]
    pad = kv_s.shape[0] - window
    c = LOG2E * HEAD ** -0.5
    scale = HEAD ** -0.5
    first = (role == 0) & (i == 0)
    rows = heads * TILE

    @pl.when(first & (b == 0))
    def _():
        kv_s[0:pad, :] = jnp.zeros((pad, 2 * HEAD), kv_s.dtype)
        kvt_s[:, 0:pad] = jnp.zeros((2 * HEAD, pad), kv_s.dtype)
        db_ref[...] = jnp.zeros_like(db_ref)

    @pl.when(first)
    def _():
        acc_s[...] = jnp.zeros_like(acc_s)
        peak = jnp.zeros((1, chip_rows), jnp.float32)
        for d, ref in enumerate((kv3_ref, kv2_ref, kv1_ref, kv0_ref)):
            part = slice(pad + d * chip_rows, pad + (d + 1) * chip_rows)
            kv_s[part, :] = ref[0]
            turned = ref[0].T
            kvt_s[:, part] = turned
            k = turned[:HEAD].astype(jnp.float32)
            peak = jnp.maximum(peak, jnp.sum(k * k, axis=0, keepdims=True))
        kn_s[...] = jnp.broadcast_to(jnp.sqrt(jnp.max(peak, axis=1, keepdims=True)), kn_s.shape)

    qt_s[...] = q_ref[0, 0].reshape(rows, HEAD).T
    dat_s[...] = da_ref[0, 0].reshape(rows, HEAD).T

    half = jnp.where(role == 0, core_ref[0], 1 - core_ref[0])
    t0 = window - chip_rows + half * (chip_rows // 2) + i * TILE
    end = t0 + TILE
    tile = (role * pl.num_programs(0) + b) * n_tiles + i
    lo_first = lo_ref[2 * tile]
    blocks = lax.div(end - lo_first + KBLK - 1, KBLK)

    def sweep(body):
        lax.fori_loop(0, lax.div(blocks, 2), lambda j, _: (body(j * (2 * KBLK), 2 * KBLK), 0)[1], 0)

        @pl.when(lax.rem(blocks, 2) == 1)
        def _():
            body((blocks - 1) * KBLK, KBLK)

    def key_rows(off, size):
        return pl.ds(pl.multiple_of(end - off - size + pad, TILE), size)

    def masked(off, size):
        s = dot(kv_s[key_rows(off, size), :HEAD], qt_s[...])
        col = t0 + lax.broadcasted_iota(jnp.int32, (size, TILE), 1)
        row = end - off - size + lax.broadcasted_iota(jnp.int32, (size, TILE), 0)
        bias = jnp.where((row <= col) & (row >= lov_ref[0, 0]), 0.0, -jnp.inf)
        return [s[:, h * TILE:(h + 1) * TILE] * c + bias for h in range(heads)]

    qf = qt_s[...].astype(jnp.float32)
    bound = jnp.sqrt(jnp.sum(qf * qf, axis=0, keepdims=True)) * (kn_s[0:1, 0:1] * (c * 1.001))
    own_keys = kvt_s[:HEAD, pl.ds(pl.multiple_of(t0 + pad, TILE), TILE)].astype(jnp.float32)
    loose = jnp.float32(0.0)
    for h in range(heads):
        cols = slice(h * TILE, (h + 1) * TILE)
        own = jnp.sum(qf[:, cols] * own_keys, axis=0, keepdims=True) * c
        loose = jnp.maximum(loose, jnp.max(bound[:, cols] - own))
    sh_s[...] = bound

    @pl.when(jnp.logical_not(loose < 80.0))
    def _():
        sh_s[...] = jnp.full_like(sh_s, -jnp.inf)

        def scan_max(j, _):
            parts = masked(j * KBLK, KBLK)
            for h in range(heads):
                cols = slice(h * TILE, (h + 1) * TILE)
                sh_s[:, cols] = jnp.maximum(sh_s[:, cols], jnp.max(parts[h], axis=0, keepdims=True))
            return 0

        lax.fori_loop(0, blocks, scan_max, 0)

    l_s[...] = jnp.zeros_like(l_s)
    o_s[...] = jnp.zeros_like(o_s)
    dq_s[...] = jnp.zeros_like(dq_s)

    def weights(off, size):
        parts = masked(off, size)
        out = pl.ds(pl.multiple_of(off, KBLK), size)
        low = []
        for h in range(heads):
            cols = slice(h * TILE, (h + 1) * TILE)
            p = jnp.exp2(parts[h] - sh_s[:, cols])
            l_s[:, cols] += fold_rows(p)
            p_s[out, cols] = p
            low.append(p.astype(jnp.bfloat16))
        o_s[...] += dot(kvt_s[HEAD:, key_rows(off, size)], jnp.concatenate(low, axis=1))

    sweep(weights)
    inv = 1.0 / jnp.sum(l_s[...], axis=0, keepdims=True)
    at = (o_s[...] * inv).astype(jnp.bfloat16)
    o_s[...] = at.astype(jnp.float32)
    l_s[0:1, :] = inv
    dl_s[...] = jnp.sum(dat_s[...].astype(jnp.float32) * o_s[...], axis=0, keepdims=True)

    def gradients(off, size):
        kr = key_rows(off, size)
        dp = dot(kv_s[kr, HEAD:], dat_s[...])
        p = p_s[pl.ds(pl.multiple_of(off, KBLK), size), :] * l_s[0:1, :]
        ds = (p * (dp - dl_s[...])).astype(jnp.bfloat16)
        p = p.astype(jnp.bfloat16)
        dq_s[...] += dot(kvt_s[:HEAD, kr], ds)
        acc_s[:HEAD, kr] += dot(qt_s[...], ds, NT)
        acc_s[HEAD:, kr] += dot(dat_s[...], p, NT)

    sweep(gradients)

    def emit(a_ref, dq_ref):
        cos_t, sin_t = cs_ref[0, 0, :HEAD // 2], cs_ref[0, 0, HEAD // 2:]
        for j in range(heads):
            cols = slice(j * TILE, (j + 1) * TILE)
            outc = slice(j * HEAD, (j + 1) * HEAD)
            a_ref[0, :, outc] = o_s[:, cols].astype(jnp.bfloat16).T
            lo_half = dq_s[:HEAD // 2, cols] * scale
            hi_half = dq_s[HEAD // 2:, cols] * scale
            back = jnp.concatenate([lo_half * cos_t + hi_half * sin_t, hi_half * cos_t - lo_half * sin_t], axis=0)
            db_ref[:, cols] += back
            dq_ref[0, :, outc] = back.astype(jnp.bfloat16).T

    @pl.when(role == 0)
    def _():
        emit(ao_ref, dqo_ref)

    @pl.when(role == 1)
    def _():
        emit(ap_ref, dqp_ref)

    @pl.when((role == 1) & (i == n_tiles - 1))
    def _():
        for d, ref in enumerate((g3_ref, g2_ref, g1_ref, g0_ref)):
            ref[0] = acc_s[:, pad + d * chip_rows:pad + (d + 1) * chip_rows]


def attention(core, lo_pair, q, da, cs, lov, kvs):
    _, n, heads, rows, _ = q.shape
    qw = heads * HEAD
    chip_rows = kvs[0].shape[1]
    window = chip_rows * len(kvs)
    n_tiles = rows // TILE
    r4 = lambda b, r, i, *_: (r, b, 0, i)
    r5 = lambda b, r, i, *_: (r, b, 0, i, 0)
    own = lambda b, r, i, *_: (b, jnp.where(r == 0, i, n_tiles - 1), 0)
    oth = lambda b, r, i, *_: (b, jnp.where(r == 0, 0, i), 0)
    whole = lambda b, r, i, *_: (b, 0, 0)
    kv_spec = pl.BlockSpec((1, chip_rows, 2 * HEAD), whole)
    head_spec = pl.BlockSpec((1, 1, heads, TILE, HEAD), r5)
    bf = jnp.bfloat16
    srows = heads * TILE
    pairs = n * 2 * rows * heads * window // 4
    nblk = window // KBLK + 1
    return pl.pallas_call(
        functools.partial(attention_kernel, heads, window),
        grid_spec=pltpu.PrefetchScalarGridSpec(
            num_scalar_prefetch=2,
            grid=(n, 2, n_tiles),
            in_specs=[head_spec, head_spec, pl.BlockSpec((1, 1, HEAD, TILE), r4), pl.BlockSpec((1, 1, 1, TILE), r4)]
            + [kv_spec] * 4,
            out_specs=[pl.BlockSpec((1, TILE, qw), own), pl.BlockSpec((1, TILE, qw), oth),
                       pl.BlockSpec((1, TILE, qw), own), pl.BlockSpec((1, TILE, qw), oth),
                       pl.BlockSpec((HEAD, srows), lambda b, r, i, *_: (0, 0))] + [pl.BlockSpec((1, 2 * HEAD, chip_rows), whole)] * 4,
            scratch_shapes=[
                pltpu.VMEM((window + TILE, 2 * HEAD), bf),
                pltpu.VMEM((2 * HEAD, window + TILE), bf),
                pltpu.VMEM((2 * HEAD, window + TILE), jnp.float32),
                pltpu.VMEM((HEAD, srows), bf),
                pltpu.VMEM((HEAD, srows), bf),
                pltpu.VMEM((nblk * KBLK, srows), jnp.float32),
                pltpu.VMEM((1, srows), jnp.float32),
                pltpu.VMEM((8, srows), jnp.float32),
                pltpu.VMEM((HEAD, srows), jnp.float32),
                pltpu.VMEM((1, srows), jnp.float32),
                pltpu.VMEM((HEAD, srows), jnp.float32),
                pltpu.VMEM((8, HEAD), jnp.float32),
            ],
        ),
        out_shape=[jax.ShapeDtypeStruct((n, rows, qw), bf)] * 4 + [jax.ShapeDtypeStruct((HEAD, srows), jnp.float32)]
        + [jax.ShapeDtypeStruct((n, 2 * HEAD, chip_rows), jnp.float32)] * 4,
        compiler_params=params(56, 3),
        cost_estimate=pl.CostEstimate(flops=pairs * 12 * HEAD * 2, bytes_accessed=n * 20_000_000 // 3, transcendentals=pairs),
        name="attention",
    )(core, lo_pair, q, da, cs, lov, *kvs)


def output_kernel(x_ref, a_ref, b_ref, wa_ref, wb_ref, y_ref):
    acc = dot(a_ref[0], wa_ref[...]) + dot(b_ref[0], wb_ref[...])
    y_ref[0] = (x_ref[0].astype(jnp.float32) + acc).astype(jnp.bfloat16)


def output(x, a, b, wa, wb):
    n, rows, width = x.shape
    blk = lambda v: pl.BlockSpec((1, rows, v.shape[2]), lambda i: (i, 0, 0))
    const = lambda v: pl.BlockSpec(v.shape, lambda i: (0, 0), pipeline_mode=pl.Buffered(1))
    return pl.pallas_call(
        output_kernel, grid=(n,), in_specs=[blk(x), blk(a), blk(b), const(wa), const(wb)], out_specs=blk(x),
        out_shape=jax.ShapeDtypeStruct(x.shape, jnp.bfloat16), compiler_params=params(40, 1),
        cost_estimate=pl.CostEstimate(flops=2 * n * rows * width * width, bytes_accessed=6 * n * rows * width, transcendentals=0),
        name="output",
    )(x, a, b, wa, wb)


def finish_kv_kernel(core_ref, p_ref, ra_ref, rb_ref, cs_ref, d_ref, db_ref):
    @pl.when((pl.program_id(0) == 0) & (pl.program_id(1) == 0))
    def _():
        db_ref[...] = jnp.zeros_like(db_ref)

    total = (p_ref[0] + ra_ref[0] + rb_ref[0]).T
    dk = unrotate(total[:, :HEAD] * (HEAD ** -0.5), cs_ref[0, 0])
    dv = total[:, HEAD:]
    d_ref[0, 0, :, :HEAD] = dk.astype(jnp.bfloat16)
    d_ref[0, 0, :, HEAD:] = dv.astype(jnp.bfloat16)
    db_ref[:, :HEAD] += fold_rows(dk)
    db_ref[:, HEAD:] += fold_rows(dv)


def finish_kv(core, part, recv_a, recv_b, cs):
    n, kw, chip_rows = part.shape
    rows = chip_rows // 2
    half = lambda r, b, c: (b, 0, jnp.where(r == 0, c[0], 1 - c[0]))
    role = lambda r, b, c: (r, b, 0, 0)
    spec = pl.BlockSpec((1, kw, rows), half)
    return pl.pallas_call(
        finish_kv_kernel,
        grid_spec=pltpu.PrefetchScalarGridSpec(
            num_scalar_prefetch=1, grid=(2, n),
            in_specs=[spec] * 3 + [pl.BlockSpec((1, 1, rows, 2 * HEAD), role)],
            out_specs=[pl.BlockSpec((1, 1, rows, kw), role), pl.BlockSpec((8, kw), lambda r, b, c: (0, 0))]),
        out_shape=[jax.ShapeDtypeStruct((2, n, rows, kw), jnp.bfloat16), jax.ShapeDtypeStruct((8, kw), jnp.float32)],
        compiler_params=params(24, 2),
        cost_estimate=pl.CostEstimate(flops=20 * n * chip_rows * kw, bytes_accessed=16 * n * chip_rows * kw, transcendentals=0),
        name="finish_kv",
    )(core, part, recv_a, recv_b, cs)


def input_grad_kernel(x_ref, g_ref, qa_ref, qb_ref, ka_ref, kb_ref, wqa_ref, wqb_ref, wka_ref, wkb_ref, gain_ref, dx_ref, dg_ref):
    @pl.when(pl.program_id(0) == 0)
    def _():
        dg_ref[...] = jnp.zeros_like(dg_ref)

    dh = (dot(qa_ref[0], wqa_ref[...], NT) + dot(qb_ref[0], wqb_ref[...], NT)
          + dot(ka_ref[0], wka_ref[...], NT) + dot(kb_ref[0], wkb_ref[...], NT))
    x = x_ref[0].astype(jnp.float32)
    inv = lax.rsqrt(jnp.mean(x * x, axis=-1, keepdims=True) + EPS)
    dg_ref[...] += fold_rows(dh * x * inv)
    e = dh * gain_ref[...]
    mean = jnp.mean(e * x, axis=-1, keepdims=True)
    dx_ref[0] = (g_ref[0].astype(jnp.float32) + inv * (e - x * (inv * inv * mean))).astype(jnp.bfloat16)


def input_grad(x, g, qa, qb, ka, kb, wqa, wqb, wka, wkb, gain):
    n, rows, width = x.shape
    blk = lambda v: pl.BlockSpec((1, rows, v.shape[2]), lambda i: (i, 0, 0))
    const = lambda v: pl.BlockSpec(v.shape, lambda i: (0, 0), pipeline_mode=pl.Buffered(1))
    ins = (x, g, qa, qb, ka, kb)
    consts = (wqa, wqb, wka, wkb, gain)
    return pl.pallas_call(
        input_grad_kernel, grid=(n,), in_specs=[blk(v) for v in ins] + [const(v) for v in consts],
        out_specs=[blk(x), pl.BlockSpec((8, width), lambda i: (0, 0))],
        out_shape=[jax.ShapeDtypeStruct(x.shape, jnp.bfloat16), jax.ShapeDtypeStruct((8, width), jnp.float32)],
        compiler_params=params(48, 1),
        cost_estimate=pl.CostEstimate(flops=2 * n * rows * width * 2048, bytes_accessed=9 * n * rows * width, transcendentals=0),
        name="input_grad",
    )(x, g, qa, qb, ka, kb, *consts)


def solution(mesh):
    cp = mesh.shape['cp']
    chips = cp // 2
    act_spec = P('dp', 'cp', None)
    tok_spec = P('dp', 'cp')
    rep_spec = P()
    mat_spec = P('dp', None)
    vec_spec = P('dp')

    def pairs(*moves):
        return [(2 * s + core, 2 * t + core) for s, t in moves for core in range(2)]

    swap_perm = [(d, d ^ 1) for d in range(cp)]
    send = lambda v, perm: lax.ppermute(v, 'cp', perm)
    swap = lambda v: send(v, swap_perm)
    kv_near = pairs(*[(s, s + 1) for s in range(chips - 1)])
    kv_mid = pairs(*[(s, s + 2) for s in range(chips - 2)])
    kv_far = pairs((0, chips - 1))
    back_near = pairs(*[(s + 1, s) for s in range(chips - 1)])
    back_mid = pairs(*[(s, s - 1) for s in range(2, chips)])
    back_far = pairs((chips - 1, 0))

    def local(x_in, grad_y, positions, seg_ids, norm_gain, w_q, b_q, w_k, b_k, w_v, b_v, w_o):
        batch, rows, width = x_in.shape
        device = lax.axis_index('cp')
        core = lax.rem(device, 2)
        core_arr = core.astype(jnp.int32).reshape(1)
        qw = width // 2
        chip_rows = 2 * rows
        window = chips * chip_rows
        half_cols = lambda w, which, size: lax.dynamic_slice_in_dim(w, which * size, size, w.ndim - 1)
        pick = lambda which: (
            half_cols(w_q, which, qw),
            jnp.concatenate([half_cols(w_k, which, HEAD), half_cols(w_v, which, HEAD)], axis=1),
            lax.dynamic_slice_in_dim(w_o, which * qw, qw, 0))
        wq_m, wkv_m, wo_m = pick(core)
        wq_t, wkv_t, wo_t = pick(1 - core)
        bq_m = half_cols(b_q, core, qw).astype(jnp.float32)[None]
        bkv_m = jnp.concatenate([half_cols(b_k, core, HEAD), half_cols(b_v, core, HEAD)]).astype(jnp.float32)[None]
        gain = norm_gain.astype(jnp.float32)[None]

        pos = jnp.stack([positions, swap(positions)])
        inv_freq = THETA ** (-jnp.arange(0, HEAD, 2).astype(jnp.float32) / HEAD)
        angles = pos.astype(jnp.float32)[..., None] * inv_freq
        cos_t, sin_t = jnp.cos(angles), jnp.sin(angles)
        cs_all = jnp.concatenate([cos_t, cos_t, -sin_t, sin_t], axis=-1)
        turned = jnp.swapaxes(angles, 2, 3)
        cst_all = jnp.concatenate([jnp.cos(turned), jnp.sin(turned)], axis=2)
        base = window - chip_rows + jnp.stack([core, 1 - core]) * rows
        lo = base[:, None, None] + jnp.arange(rows) - pos
        lo_tiles = lo.reshape(2, batch, rows // TILE, TILE)
        lo_pair_all = jnp.stack([lo_tiles[..., 0], lo_tiles[..., -1]], axis=-1)

        n_chunks = batch // CHUNK
        cut = lambda v, c: v[c * CHUNK:(c + 1) * CHUNK]
        cut1 = lambda v, c: v[:, c * CHUNK:(c + 1) * CHUNK]
        xs = [cut(x_in, c) for c in range(n_chunks)]
        gs = [cut(grad_y, c) for c in range(n_chunks)]
        y_parts, dx_parts, outs = [], [], []
        dwq = dwo = dwkv = None
        db_q = jnp.zeros((HEAD, qw), jnp.float32)
        db_kv = jnp.zeros((8, 2 * HEAD), jnp.float32)
        dgain = jnp.zeros((8, width), jnp.float32)
        add = lambda a, b: b if a is None else a + b
        tn = lambda a, b: jnp.einsum('nte,ntd->ed', a, b, preferred_element_type=jnp.float32)
        proj = []
        for c in range(n_chunks):
            x_oth, g_oth = swap(xs[c]), swap(gs[c])
            cs = cut1(cs_all, c)
            h, q, da, kv = projection(core_arr, xs[c], x_oth, gs[c], g_oth, cs, gain, wq_m, wkv_m, wo_m, bq_m, bkv_m)
            kvs = [kv, send(kv, kv_near), send(kv, kv_mid), send(kv, kv_far)]
            proj.append((h, q, da, cs, kvs, g_oth))
        for c in range(n_chunks):
            h, q, da, cs, kvs, g_oth = proj[c]
            lo_c = cut1(lo, c)[:, :, None]
            pair_c = cut1(lo_pair_all, c).reshape(-1)
            a_own, a_oth, dq_own, dq_oth, dbq_c, g0, g1, g2, g3 = attention(core_arr, pair_c, q, da, cut1(cst_all, c), lo_c, kvs)
            db_q = db_q + dbq_c
            far = send(g3, back_far)
            mid = send(g2, back_mid)
            near = send(g1 + mid, back_near)
            a_got, dq_got = swap(a_oth), swap(dq_oth)
            y_parts.append(output(xs[c], a_own, a_got, wo_m, wo_t))
            dwo = add(dwo, tn(a_own, gs[c]) + tn(a_oth, g_oth))
            dwq = add(dwq, tn(h[0], dq_own) + tn(h[1], dq_oth))
            dkv, dbkv_c = finish_kv(core_arr, g0, near, far, cs)
            db_kv = db_kv + dbkv_c
            dkv_got = swap(dkv[1])
            dwkv = add(dwkv, tn(h[0], dkv[0]) + tn(h[1], dkv[1]))
            dx_c, dg_c = input_grad(xs[c], gs[c], dq_own, dq_got, dkv[0], dkv_got, wq_m, wq_t, wkv_m, wkv_t, gain)
            dx_parts.append(dx_c)
            dgain = dgain + dg_c
        y_out = jnp.concatenate(y_parts)
        dx = jnp.concatenate(dx_parts)

        groups = [[2 * k + co for k in range(chips)] for co in range(2)]
        psum4 = lambda v: lax.psum(v, 'cp', axis_index_groups=groups)
        order = lambda mine, theirs, ax: jnp.where(core == 0, jnp.concatenate([mine, theirs], ax), jnp.concatenate([theirs, mine], ax))
        dwo_s = psum4(dwo)
        grad_w_o = order(dwo_s, swap(dwo_s), 0)
        dwq_s = psum4(dwq)
        grad_w_q = order(dwq_s, swap(dwq_s), 1)
        dwkv_s = psum4(dwkv)
        dwkv_t = swap(dwkv_s)
        grad_w_k = order(dwkv_s[:, :HEAD], dwkv_t[:, :HEAD], 1)
        grad_w_v = order(dwkv_s[:, HEAD:], dwkv_t[:, HEAD:], 1)
        small = jnp.concatenate([jnp.sum(db_q.reshape(HEAD, qw // HEAD, HEAD), 2).T.reshape(-1), jnp.sum(db_kv, 0)])
        both = jnp.zeros((2, small.shape[0]), jnp.float32)
        both = lax.dynamic_update_slice(both, small[None], (core, 0))
        vec = lax.psum(jnp.concatenate([both.reshape(-1), jnp.sum(dgain, 0)]), 'cp')
        both = vec[:2 * small.shape[0]].reshape(2, -1)
        grad_b_q = both[:, :qw].reshape(-1)
        grad_b_k = both[:, qw:qw + HEAD].reshape(-1)
        grad_b_v = both[:, qw + HEAD:].reshape(-1)
        grad_gain = vec[2 * small.shape[0]:]
        return y_out, dx, grad_gain, grad_w_q, grad_b_q, grad_w_k, grad_b_k, grad_w_v, grad_b_v, grad_w_o

    in_specs = (act_spec, act_spec, tok_spec, tok_spec) + (rep_spec,) * 8
    out_specs = (act_spec, act_spec, vec_spec, mat_spec, vec_spec, mat_spec, vec_spec, mat_spec, vec_spec, mat_spec)
    return jax.shard_map(local, mesh=mesh, in_specs=in_specs, out_specs=out_specs, check_vma=False)
```
